32 devices in a mesh: prow: 4 (over y, x), pcol: 8 (over z, core).
Axes of the slice: x: 2, y: 2, z: 4, core: 2. Of those that a mesh axis runs over, the one named last changes fastest.
Arguments:
- matrix: float32 [16, 4, 256, 8, 8, 256], P(None, 'prow', None, None, 'pcol'), may hold values from -6 to 6, as said below
- factor: float32 [16, 4, 256, 8, 8, 256], P(None, 'prow', None, None, 'pcol'), may hold values from -3 to 3, as said below
Outputs:
- reduced: float32 [16, 4, 256, 8, 8, 256], P(None, 'prow', None, None, 'pcol')
The draws below stay inside these ranges and needn't reach their ends.
Inputs may be any that keep to these rules, and one draw needn't show every extreme that they name: Symmetric matrix stored in its lower triangle: every entry above the diagonal is zero. `factor`: lower triangular with diagonal entries between 1 and 3; every entry above the diagonal is zero.
All inputs are finite; a program needn't handle non-finite values.
Results may differ from the reference program's by a relative error of at most 0.0001.
Values sent between devices are 32-bit elements; how exact they have to be, the bound alone decides.
A program may use at most 256 MiB of HBM per device.

```python
import jax
import jax.numpy as jnp
from jax import lax

ORDER = 16384
NB = 256
BLOCKS = 2
RT = 16
CT = 8


def draw_matrix(key, part):
    rows = jnp.arange(ORDER, dtype=jnp.int32)[:, None]
    cols = jnp.arange(ORDER, dtype=jnp.int32)[None, :]
    values = jnp.clip(jax.random.normal(key, (ORDER, ORDER), jnp.float32), -6.0, 6.0)
    values = jnp.where(rows >= cols, values, 0.0)
    return values.reshape(RT, ORDER // (RT * NB), NB, CT, ORDER // (CT * NB), NB)


def draw_factor(key, part):
    first, second = jax.random.split(jax.random.fold_in(key, 7))
    rows = jnp.arange(ORDER, dtype=jnp.int32)[:, None]
    cols = jnp.arange(ORDER, dtype=jnp.int32)[None, :]
    same_tile = rows // NB == cols // NB
    spread = jnp.where(same_tile, 0.5, 0.3) / jnp.sqrt(jnp.float32(NB))
    noise = jnp.clip(jax.random.normal(first, (ORDER, ORDER), jnp.float32), -5.0, 5.0)
    diagonal = jnp.exp(jax.random.uniform(second, (ORDER,), jnp.float32, 0.0, jnp.log(3.0)))
    values = jnp.where(rows > cols, noise * spread, 0.0) + jnp.where(rows == cols, diagonal[:, None], 0.0)
    return values.reshape(RT, ORDER // (RT * NB), NB, CT, ORDER // (CT * NB), NB)


def setup_inputs(seed: int = 0) -> dict:
    keys = jax.random.split(jax.random.key(seed), 3)
    return {
        "matrix": draw_matrix(jax.random.fold_in(keys[2], 71), 0),
        "factor": draw_factor(jax.random.fold_in(keys[2], 71), 0),
    }


highest = lax.Precision.HIGHEST

def product(left, right):
    return jnp.dot(left.astype(jnp.float32), right.astype(jnp.float32), precision=highest, preferred_element_type=jnp.float32)

def product_trans(left, right):
    return lax.dot_general(left.astype(jnp.float32), right.astype(jnp.float32), (((1,), (1,)), ((), ())), precision=highest, preferred_element_type=jnp.float32)

def diagonal_core(diag_block, diag_factor, width):
    identity = jnp.eye(width, dtype=jnp.float32)
    inverse = lax.linalg.triangular_solve(diag_factor, identity, left_side=True, lower=True)
    symmetric = diag_block + diag_block.T - jnp.diag(jnp.diagonal(diag_block))
    inner = product_trans(product(inverse, symmetric), inverse)
    return (inverse, 0.5 * (inner + inner.T))

def reference(matrix, factor):
    full = matrix.reshape(ORDER, ORDER)
    lower = factor.reshape(ORDER, ORDER)
    for step in range(BLOCKS):
        low = step * NB
        high = low + NB
        inverse, core = diagonal_core(full[low:high, low:high], lower[low:high, low:high], NB)
        panel = full[high:, low:high]
        factor_panel = lower[high:, low:high]
        shared = product(factor_panel, core)
        halfway = product_trans(panel, inverse) - 0.5 * shared
        finished = halfway - 0.5 * shared
        update = product_trans(halfway, factor_panel) + product_trans(factor_panel, halfway)
        trailing = full[high:, high:] - jnp.tril(update)
        full = full.at[high:, high:].set(trailing)
        full = full.at[low:high, low:high].set(jnp.tril(core))
        full = full.at[high:, low:high].set(finished)
    return full.reshape(RT, ORDER // (RT * NB), NB, CT, ORDER // (CT * NB), NB)
```

```python
import functools

import jax
import jax.numpy as jnp
from jax import lax
from jax.experimental import pallas as pl
from jax.experimental.pallas import tpu as pltpu
from jax.sharding import PartitionSpec as P

MESH = pl.DeviceIdType.MESH
CORES = 2
LAG = 2
LIMIT = 60 * 1024 * 1024

highest = lax.Precision.HIGHEST


def dot(left, right):
    return jnp.dot(left, right, precision=highest, preferred_element_type=jnp.float32)


def dot_trans(left, right, precision=highest):
    return lax.dot_general(
        left, right, (((1,), (1,)), ((), ())), precision=precision, preferred_element_type=jnp.float32
    )


def grid_of(count):
    across = 1
    while across * across * 4 <= count:
        across *= 2
    return count // across, across


def gather_kernel(
    prows, pcols, matrix, factor, row_out, col_out, fin_out,
    rows, cols, panel, corner, inverse, core, half,
    load_sem, row_recv, col_recv, corner_recv, corner_send,
    down_send, side_send, col_send, relay_send, out_sem,
):
    row_tiles, _, width, _ = rows.shape
    col_tiles = cols.shape[0]
    high, across = grid_of(prows)
    depth = pcols // CORES
    ratio = pcols // prows
    prow = lax.axis_index("prow")
    pcol = lax.axis_index("pcol")
    plane = pcol // CORES
    side = pcol % CORES
    y, x = prow // across, prow % across
    top = plane == 0

    barrier = pltpu.get_barrier_semaphore()

    def greet(where):
        pl.semaphore_signal(barrier, inc=1, device_id=where, device_id_type=MESH)

    def greet_plane(index, _):
        other = (index // CORES, plane * CORES + index % CORES)

        @pl.when(index != prow * CORES + side)
        def _():
            greet(other)

        return 0

    lax.fori_loop(0, prows * CORES, greet_plane, 0)

    @pl.when(plane > 0)
    def _():
        greet((prow, pcol - CORES))

    @pl.when(plane < depth - 1)
    def _():
        greet((prow, pcol + CORES))

    greeted = prows * CORES - 1 + jnp.where(plane > 0, 1, 0) + jnp.where(plane < depth - 1, 1, 0)
    pl.semaphore_wait(barrier, greeted)

    def remote(source, target, send, recv, where):
        return pltpu.make_async_remote_copy(
            src_ref=source, dst_ref=target, send_sem=send, recv_sem=recv, device_id=where, device_id_type=MESH
        )

    def down_copy(i, late):
        kind = side + CORES * late
        return remote(
            rows.at[i, kind], rows.at[i, kind], down_send.at[i, late], row_recv.at[i, kind], (prow, pcol + CORES)
        )

    def side_copy(i, late, kind):
        return remote(
            rows.at[i, kind], rows.at[i, kind], side_send.at[i, late], row_recv.at[i, kind],
            (prow, plane * CORES + 1 - side),
        )

    def ways(source):
        ys, xs = source // across, source % across
        return (
            ((x == xs) & (y >= ys) & (y + 1 < high), prow + across),
            ((x == xs) & (y <= ys) & (y >= 1), prow - across),
            ((x >= xs) & (x + 1 < across), prow + 1),
            ((x <= xs) & (x >= 1), prow - 1),
        )

    def for_columns(i, late, act):
        kind = side + CORES * late
        for other in range(CORES):
            column = plane * CORES + other
            first = column // prows
            j = (i - first) // ratio

            @pl.when((column % prows == prow) & (i >= first) & ((i - first) % ratio == 0))
            def _():
                for way, (fits, where) in enumerate(ways(prow)):
                    @pl.when(fits)
                    def _():
                        act(remote(
                            rows.at[i, kind], cols.at[j, kind], col_send.at[other, way, i, late],
                            col_recv.at[j, kind], (where, column),
                        ))

    def emit(i, late):
        @pl.when(plane < depth - 1)
        def _():
            down_copy(i, late).start()

        side_copy(i, late, side + CORES * late).start()
        for_columns(i, late, lambda copy: copy.start())

    source = pcol % prows
    first_tile = pcol // prows

    def for_relay(i, late, act):
        j = (i - first_tile) // ratio

        @pl.when((prow != source) & (i >= first_tile) & ((i - first_tile) % ratio == 0))
        def _():
            for kind in (CORES * late, CORES * late + 1):
                act(j, kind)

    def relay_copies(j, kind, act):
        for way, (fits, where) in enumerate(ways(source)):
            @pl.when(fits)
            def _():
                act(remote(
                    cols.at[j, kind], cols.at[j, kind], relay_send.at[way, j, kind], col_recv.at[j, kind],
                    (where, pcol),
                ))

    def arrive_column(j, kind):
        remote(
            cols.at[j, kind], cols.at[j, kind], relay_send.at[0, j, kind], col_recv.at[j, kind], (prow, pcol)
        ).wait_recv()
        relay_copies(j, kind, lambda copy: copy.start())

    def relay(i, late):
        for_relay(i, late, arrive_column)

    def load(which, i):
        if which == 0:
            return pltpu.make_async_copy(factor.at[i, 0, :, 0, 0, :], rows.at[i, side], load_sem.at[0, i])
        return pltpu.make_async_copy(matrix.at[i, 0, :, 0, 0, :], panel.at[i], load_sem.at[1, i])

    owner = top & (prow < 2) & (side <= prow)
    slot = 2 * (prow + side)

    def corner_copy(which, index):
        sent = panel.at[0] if which == 0 else rows.at[0, side]
        return remote(
            sent, corner.at[slot + which], corner_send.at[which, index], corner_recv.at[slot + which],
            (index // CORES, index % CORES),
        )

    def each_peer(act):
        def body(index, _):
            @pl.when(index != prow * CORES + side)
            def _():
                for which in range(2):
                    act(corner_copy(which, index))
            return 0
        lax.fori_loop(0, prows * CORES, body, 0)

    row_id = lax.broadcasted_iota(jnp.int32, (width, width), 0)
    col_id = lax.broadcasted_iota(jnp.int32, (width, width), 1)

    @pl.when(top)
    def _():
        def start_loads(i, _):
            load(1, i).start()
            load(0, i).start()
            return 0
        lax.fori_loop(0, row_tiles, start_loads, 0)
        load(1, 0).wait()
        load(0, 0).wait()

        @pl.when(owner)
        def _():
            each_peer(lambda copy: copy.start())
            corner[slot] = panel[0]
            corner[slot + 1] = rows[0, side]

        emit(0, 0)

        def send_early(i, _):
            load(0, i).wait()
            emit(i, 0)
            return 0
        lax.fori_loop(1, row_tiles, send_early, 0)

        def await_corner(index, _):
            @pl.when(jnp.logical_not(owner & ((index == slot) | (index == slot + 1))))
            def _():
                remote(
                    corner.at[index], corner.at[index], corner_send.at[0, 0], corner_recv.at[index], (prow, pcol)
                ).wait_recv()
            return 0
        lax.fori_loop(0, 6, await_corner, 0)

        levels = (width - 1).bit_length()

        def invert(step, _):
            lower = corner[1 + 4 * step]
            diagonal = row_id == col_id
            inverse[step] = jnp.where(diagonal, 1.0 / jnp.where(diagonal, lower, 1.0), 0.0)

            def level(bit, _):
                block = lax.shift_right_logical(row_id, bit)
                under = (block % 2 == 1) & (lax.shift_right_logical(col_id, bit) == block - 1)
                now = inverse[step]
                cross = jnp.where(under, corner[1 + 4 * step], 0.0)
                inverse[step] = now - dot(dot(now, cross), now)
                return 0
            lax.fori_loop(0, levels, level, 0)
            return 0
        lax.fori_loop(0, 2, invert, 0)

        def core_of(block, inv):
            symmetric = block + block.T - jnp.where(row_id == col_id, block, 0.0)
            inner = dot_trans(dot(inv, symmetric), inv)
            return 0.5 * (inner + inner.T)

        core[0] = core_of(corner[0], inverse[0])
        half[...] = dot_trans(corner[2], inverse[0]) - 0.5 * dot(corner[3], core[0])
        cross = dot_trans(half[...], corner[3]) + dot_trans(corner[3], half[...])
        corner[4] = corner[4] - jnp.where(row_id >= col_id, cross, 0.0)
        core[1] = core_of(corner[4], inverse[1])

        @pl.when(owner)
        def _():
            each_peer(lambda copy: copy.wait_send())

    @pl.when(jnp.logical_not(top))
    def _():
        def pass_early(i, _):
            down_copy(i, 0).wait_recv()
            emit(i, 0)
            relay(i - LAG, 0)
            return 0
        lax.fori_loop(0, row_tiles, pass_early, 0)

    def reduce_tile(i):
        @pl.when(i > 0)
        def _():
            load(1, i).wait()

        @pl.when(side == 1)
        def _():
            for late in range(2):
                side_copy(i, late, 2 * late).wait_recv()
            panel[i] = (
                panel[i] - dot_trans(rows[i, 2], corner[3]) - dot_trans(rows[i, 0], half[...])
            )

        shared = dot(rows[i, side], core[side])
        halfway = dot_trans(panel[i], inverse[side]) - 0.5 * shared
        rows[i, side + 2] = halfway
        tile = i * prows + prow
        lower = jnp.where(row_id >= col_id, core[side], 0.0)
        final = halfway - 0.5 * shared
        final = jnp.where(tile > side, final, jnp.where(tile == side, lower, 0.0))
        panel[i] = final

    def late_step(i, _):
        @pl.when(top & (i < row_tiles))
        def _():
            reduce_tile(i)

        @pl.when(i >= 1)
        def _():
            @pl.when(jnp.logical_not(top))
            def _():
                down_copy(i - 1, 1).wait_recv()
            emit(i - 1, 1)

        @pl.when(top & (i < row_tiles))
        def _():
            relay(i, 0)

        @pl.when(jnp.logical_not(top) & (i < LAG))
        def _():
            relay(row_tiles - LAG + i, 0)

        relay(i - 1 - LAG, 1)
        return 0
    lax.fori_loop(0, row_tiles + 1, late_step, 0)
    for back in range(LAG):
        relay(row_tiles - LAG + back, 1)

    def await_side(i, _):
        @pl.when(jnp.logical_not(top & (side == 1)))
        def _():
            for late in range(2):
                side_copy(i, late, 1 - side + 2 * late).wait_recv()
        return 0
    lax.fori_loop(0, row_tiles, await_side, 0)

    outs = (
        pltpu.make_async_copy(rows, row_out, out_sem.at[0]),
        pltpu.make_async_copy(cols, col_out, out_sem.at[1]),
        pltpu.make_async_copy(panel, fin_out, out_sem.at[2]),
    )
    outs[0].start()

    @pl.when(prow != source)
    def _():
        outs[1].start()

    @pl.when(top)
    def _():
        outs[2].start()

    def drain(i, _):
        for late in range(2):
            @pl.when(plane < depth - 1)
            def _():
                down_copy(i, late).wait_send()
            side_copy(i, late, side + 2 * late).wait_send()
            for_columns(i, late, lambda copy: copy.wait_send())
            for_relay(i, late, lambda j, kind: relay_copies(j, kind, lambda copy: copy.wait_send()))
        return 0
    lax.fori_loop(0, row_tiles, drain, 0)

    outs[0].wait()

    @pl.when(prow != source)
    def _():
        outs[1].wait()

    @pl.when(top)
    def _():
        outs[2].wait()


def split(value):
    high = value.astype(jnp.bfloat16)
    return high, (value - high.astype(jnp.float32)).astype(jnp.bfloat16)


def update_kernel(
    prows, pcols, matrix, row_in, col_in, fin_in, out,
    rows, row_high, row_low, staged, col_high, col_low, tiles, zeros,
    row_sem, col_sem, in_sem, out_sem,
):
    row_tiles = row_in.shape[0]
    col_tiles, _, width, _ = col_in.shape
    ratio = pcols // prows
    prow = lax.axis_index("prow")
    pcol = lax.axis_index("pcol")
    source = pcol % prows
    first_tile = pcol // prows
    fixed = pcol < 2
    row_id = lax.broadcasted_iota(jnp.int32, (width, width), 0)
    col_id = lax.broadcasted_iota(jnp.int32, (width, width), 1)
    zeros[...] = jnp.zeros_like(zeros)

    def row_copy(i):
        return pltpu.make_async_copy(row_in.at[i], rows.at[i % 2], row_sem.at[i % 2])

    def col_start(j):
        @pl.when(prow == source)
        def _():
            pltpu.make_async_copy(row_in.at[ratio * j + first_tile], staged.at[j % 2], col_sem.at[j % 2]).start()

        @pl.when(prow != source)
        def _():
            pltpu.make_async_copy(col_in.at[j], staged.at[j % 2], col_sem.at[j % 2]).start()

    def live(i, j):
        return j * pcols + pcol <= i * prows + prow

    def is_fixed(j):
        return fixed & (j == 0)

    def start_loads(i):
        def body(j, _):
            @pl.when(live(i, j) & jnp.logical_not(is_fixed(j)))
            def _():
                pltpu.make_async_copy(matrix.at[i, 0, :, j, 0, :], tiles.at[i % 3, j], in_sem.at[i % 3, j]).start()

            @pl.when(live(i, j) & is_fixed(j))
            def _():
                pltpu.make_async_copy(fin_in.at[i], tiles.at[i % 3, j], in_sem.at[i % 3, j]).start()
            return 0
        lax.fori_loop(0, col_tiles, body, 0)

    def out_copy(i, j):
        return pltpu.make_async_copy(tiles.at[i % 3, j], out.at[i, 0, :, j, 0, :], out_sem.at[i % 3, j])

    def zero_copy(i, j):
        return pltpu.make_async_copy(zeros, out.at[i, 0, :, j, 0, :], out_sem.at[i % 3, j])

    def wait_outs(i):
        def body(j, _):
            out_copy(i, j).wait()
            return 0
        lax.fori_loop(0, col_tiles, body, 0)

    col_start(0)
    row_copy(0).start()
    start_loads(0)

    def prepare(j, _):
        @pl.when(j + 1 < col_tiles)
        def _():
            col_start(j + 1)
        pltpu.make_async_copy(col_in.at[j], staged.at[j % 2], col_sem.at[j % 2]).wait()
        for kind in range(4):
            upper, lower = split(staged[j % 2, kind])
            place = pl.ds((kind + 2) % 4 * width, width)
            col_high[j, :, place] = upper
            col_low[j, :, place] = lower
        return 0
    lax.fori_loop(0, col_tiles, prepare, 0)

    def row_step(i, _):
        @pl.when(i >= 2)
        def _():
            wait_outs(i - 2)

        @pl.when(i + 1 < row_tiles)
        def _():
            row_copy(i + 1).start()
            start_loads(i + 1)
        row_copy(i).wait()
        for kind in range(4):
            upper, lower = split(rows[i % 2, kind])
            row_high[:, kind * width:(kind + 1) * width] = upper
            row_low[:, kind * width:(kind + 1) * width] = lower

        def tile_step(j, _):
            @pl.when(live(i, j))
            def _():
                pltpu.make_async_copy(zeros, tiles.at[i % 3, j], in_sem.at[i % 3, j]).wait()

                @pl.when(jnp.logical_not(is_fixed(j)))
                def _():
                    total = (
                        dot_trans(row_high[...], col_low[j], None)
                        + dot_trans(row_low[...], col_high[j], None)
                        + dot_trans(row_high[...], col_high[j], None)
                    )
                    gap = ((i * prows + prow) - (j * pcols + pcol)) * width
                    tiles[i % 3, j] = tiles[i % 3, j] - jnp.where(row_id + gap >= col_id, total, 0.0)
                out_copy(i, j).start()

            @pl.when(jnp.logical_not(live(i, j)))
            def _():
                zero_copy(i, j).start()
            return 0
        lax.fori_loop(0, col_tiles, tile_step, 0)
        return 0
    lax.fori_loop(0, row_tiles, row_step, 0)
    for back in range(min(2, row_tiles), 0, -1):
        wait_outs(row_tiles - back)


def on_device(matrix, factor):
    row_tiles, _, width, col_tiles, _, _ = matrix.shape
    prows = lax.axis_size("prow")
    pcols = lax.axis_size("pcol")
    tile = (width, width)
    f32 = jnp.float32
    anywhere = pl.BlockSpec(memory_space=pl.ANY)
    dma = pltpu.SemaphoreType.DMA
    row_all, col_all, fin = pl.pallas_call(
        functools.partial(gather_kernel, prows, pcols),
        out_shape=(
            jax.ShapeDtypeStruct((row_tiles, 4) + tile, f32),
            jax.ShapeDtypeStruct((col_tiles, 4) + tile, f32),
            jax.ShapeDtypeStruct((row_tiles,) + tile, f32),
        ),
        in_specs=[anywhere, anywhere],
        out_specs=(anywhere, anywhere, anywhere),
        scratch_shapes=[
            pltpu.VMEM((row_tiles, 4) + tile, f32),
            pltpu.VMEM((col_tiles, 4) + tile, f32),
            pltpu.VMEM((row_tiles,) + tile, f32),
            pltpu.VMEM((6,) + tile, f32),
            pltpu.VMEM((2,) + tile, f32),
            pltpu.VMEM((2,) + tile, f32),
            pltpu.VMEM(tile, f32),
            dma((2, row_tiles)),
            dma((row_tiles, 4)),
            dma((col_tiles, 4)),
            dma((6,)),
            dma((2, prows * CORES)),
            dma((row_tiles, 2)),
            dma((row_tiles, 2)),
            dma((CORES, 4, row_tiles, 2)),
            dma((4, col_tiles, 4)),
            dma((3,)),
        ],
        compiler_params=pltpu.CompilerParams(collective_id=0, has_side_effects=True, vmem_limit_bytes=LIMIT),
        name="gather",
    )(matrix, factor)
    return pl.pallas_call(
        functools.partial(update_kernel, prows, pcols),
        out_shape=jax.ShapeDtypeStruct(matrix.shape, f32),
        in_specs=[anywhere] * 4,
        out_specs=anywhere,
        scratch_shapes=[
            pltpu.VMEM((2, 4) + tile, f32),
            pltpu.VMEM((width, 4 * width), jnp.bfloat16),
            pltpu.VMEM((width, 4 * width), jnp.bfloat16),
            pltpu.VMEM((2, 4) + tile, f32),
            pltpu.VMEM((col_tiles, width, 4 * width), jnp.bfloat16),
            pltpu.VMEM((col_tiles, width, 4 * width), jnp.bfloat16),
            pltpu.VMEM((3, col_tiles) + tile, f32),
            pltpu.VMEM(tile, f32),
            dma((2,)),
            dma((2,)),
            dma((3, col_tiles)),
            dma((3, col_tiles)),
        ],
        compiler_params=pltpu.CompilerParams(vmem_limit_bytes=LIMIT),
        name="update",
    )(matrix, row_all, col_all, fin)


def solution(mesh):
    placed = P(None, "prow", None, None, "pcol", None)
    return jax.shard_map(on_device, mesh=mesh, in_specs=(placed, placed), out_specs=placed, check_vma=False)
```

```python
import functools

import jax
import jax.numpy as jnp
from jax import lax
from jax.experimental import pallas as pl
from jax.experimental.pallas import tpu as pltpu
from jax.sharding import PartitionSpec as P

MESH = pl.DeviceIdType.MESH
CORES = 2
NEAR = 2
FAR = 3
SENT = 4
EARLY_NEAR = 3
EARLY_FAR = 6
PARTS = 4
LIMIT = 60 * 1024 * 1024

highest = lax.Precision.HIGHEST


def dot(left, right):
    return jnp.dot(left, right, precision=highest, preferred_element_type=jnp.float32)


def dot_trans(left, right, precision=highest):
    return lax.dot_general(
        left, right, (((1,), (1,)), ((), ())), precision=precision, preferred_element_type=jnp.float32
    )


def grid_of(count):
    across = 1
    while across * across * 4 <= count:
        across *= 2
    return count // across, across


def lanes_of(prows):
    return 2 if max(grid_of(prows)) <= 2 else 4


def early_pairs(row_tiles):
    return max(1, row_tiles // 2 * 7 // 8)


def pair_columns(pair, ratio):
    return (2 * pair + 1) // ratio + 1


def split(value):
    high = value.astype(jnp.bfloat16)
    return high, (value - high.astype(jnp.float32)).astype(jnp.bfloat16)


def split_rows(first, second, row_high, row_low):
    width = first.shape[-1]
    for place, tiles in enumerate((first, second)):
        for kind in range(4):
            upper, lower = split(tiles[kind])
            row_high[place * width:(place + 1) * width, kind * width:(kind + 1) * width] = upper
            row_low[place * width:(place + 1) * width, kind * width:(kind + 1) * width] = lower


def split_column(tiles, high, low):
    width = tiles.shape[-1]
    for kind in range(4):
        upper, lower = split(tiles[kind])
        place = (kind + 2) % 4 * width
        high[:, place:place + width] = upper
        low[:, place:place + width] = lower


def subtract_update(tiles, row_high, row_low, high, low, row_tile, prows, col_tile):
    width = tiles.shape[-1]
    total = (
        dot_trans(row_high[...], low[...], None)
        + dot_trans(row_low[...], high[...], None)
        + dot_trans(row_high[...], high[...], None)
    )
    row_id = lax.broadcasted_iota(jnp.int32, (width, width), 0)
    col_id = lax.broadcasted_iota(jnp.int32, (width, width), 1)
    for place in range(2):
        gap = (row_tile + place * prows - col_tile) * width
        part = total[place * width:(place + 1) * width]
        tiles[place] = tiles[place] - jnp.where(row_id + gap >= col_id, part, 0.0)


def gather_kernel(
    prows, pcols, matrix, factor, row_out, high_out, low_out, fin_out, done_out,
    rows, cols, panel, corner, inverse, core, half, row_high, row_low, col_high, col_low, tiles,
    load_sem, down_recv, side_recv, col_recv, col_fine, corner_recv, corner_send,
    down_send, side_send, col_send, send_fine, relay_send, relay_fine, out_sem, row_sem, column_sem, tile_load, tile_out,
):
    row_tiles, _, width, _ = rows.shape
    col_tiles = cols.shape[0]
    high, across = grid_of(prows)
    depth = pcols // CORES
    ratio = pcols // prows
    prow = lax.axis_index("prow")
    pcol = lax.axis_index("pcol")
    plane = pcol // CORES
    side = pcol % CORES
    y, x = prow // across, prow % across
    top = plane == 0

    barrier = pltpu.get_barrier_semaphore()

    def greet(where):
        pl.semaphore_signal(barrier, inc=1, device_id=where, device_id_type=MESH)

    def greet_plane(index, _):
        other = (index // CORES, plane * CORES + index % CORES)

        @pl.when(index != prow * CORES + side)
        def _():
            greet(other)

        return 0

    lax.fori_loop(0, prows * CORES, greet_plane, 0)

    @pl.when(plane > 0)
    def _():
        greet((prow, pcol - CORES))

    @pl.when(plane < depth - 1)
    def _():
        greet((prow, pcol + CORES))

    greeted = prows * CORES - 1 + jnp.where(plane > 0, 1, 0) + jnp.where(plane < depth - 1, 1, 0)
    pl.semaphore_wait(barrier, greeted)

    def remote(source, target, send, recv, where):
        return pltpu.make_async_remote_copy(
            src_ref=source, dst_ref=target, send_sem=send, recv_sem=recv, device_id=where, device_id_type=MESH
        )

    chunk = width // PARTS
    lanes = lanes_of(prows)
    work_lag = 3 if ratio > 1 else 5

    def span(part):
        return pl.ds(pl.multiple_of(part * chunk, chunk), chunk)

    def by_parts(i, late, part, whole, piece):
        fine = (i >= row_tiles - ratio) & (late == 1)

        @pl.when(fine)
        def _():
            piece()

        @pl.when(jnp.logical_not(fine) & (part == PARTS - 1))
        def _():
            whole()

    def down_copy(i, late, part):
        piece = rows.at[i, side + CORES * late, span(part)]
        return remote(
            piece, piece, down_send.at[i, late], down_recv.at[i, late, part], (prow, pcol + CORES)
        )

    def side_copy(i, late, kind):
        return remote(
            rows.at[i, kind], rows.at[i, kind], side_send.at[i, late], side_recv.at[i, late],
            (prow, plane * CORES + 1 - side),
        )

    def ways(source):
        ys, xs = source // across, source % across
        return (
            ((x == xs) & (y >= ys) & (y + 1 < high), prow + across),
            ((x == xs) & (y <= ys) & (y >= 1), prow - across),
            ((x >= xs) & (x + 1 < across), prow + 1),
            ((x <= xs) & (x >= 1), prow - 1),
        )

    def for_columns(i, late, part, act):
        kind = side + CORES * late
        for other in range(CORES):
            column = plane * CORES + other
            first = column // prows
            j = (i - first) // ratio

            @pl.when((column % prows == prow) & (i >= first) & ((i - first) % ratio == 0))
            def _():
                for way, (fits, where) in enumerate(ways(prow)):
                    @pl.when(fits)
                    def _():
                        lane = way * lanes // 4
                        by_parts(
                            i, late, part,
                            lambda: act(remote(
                                rows.at[i, kind], cols.at[j, kind], col_send.at[lane, j, late],
                                col_recv.at[j, kind], (where, column),
                            )),
                            lambda: act(remote(
                                rows.at[i, kind, span(part)], cols.at[j, kind, span(part)],
                                send_fine.at[lane, part], col_fine.at[side, part], (where, column),
                            )),
                        )

    def pass_down(i, late, part):
        @pl.when(jnp.logical_not(top))
        def _():
            down_copy(i, late, part).wait_recv()

        @pl.when(plane < depth - 1)
        def _():
            down_copy(i, late, part).start()

        @pl.when((part == PARTS - 1) | ((i >= row_tiles - ratio) & (late == 1)))
        def _():
            for_columns(i, late, part, lambda copy: copy.start())

    def pass_whole(i, late):
        def body(part, _):
            pass_down(i, late, part)
            return 0
        lax.fori_loop(0, PARTS, body, 0)

    def emit(i, late):
        side_copy(i, late, side + CORES * late).start()

    source = pcol % prows
    first_tile = pcol // prows
    far = (x != source % across) & (y != source // across)
    lag = jnp.where(far, FAR, NEAR)
    bridge = (x == source % across) & (y != source // across)
    early_lag = jnp.where(far, min(EARLY_FAR, row_tiles), min(EARLY_NEAR, row_tiles))

    def for_relay(i, late, act):
        j = (i - first_tile) // ratio

        @pl.when((prow != source) & (i >= first_tile) & (i < row_tiles) & ((i - first_tile) % ratio == 0))
        def _():
            def body(part, _):
                for kind in (CORES * late, CORES * late + 1):
                    by_parts(
                        i, late, part,
                        lambda: act(kind, cols.at[j, kind], relay_send.at[:, j, kind], col_recv.at[j, kind]),
                        lambda: act(
                            kind, cols.at[j, kind, span(part)],
                            relay_fine.at[:, kind % CORES, part], col_fine.at[kind % CORES, part],
                        ),
                    )
                return 0
            lax.fori_loop(0, PARTS, body, 0)

    def relay_copies(piece, send, recv, act):
        for way, (fits, where) in enumerate(ways(source)):
            @pl.when(fits)
            def _():
                act(remote(
                    piece, piece, send.at[way * lanes // 4], recv, (where, pcol),
                ))

    def arrive_column(kind, piece, send, recv):
        remote(piece, piece, send.at[0], recv, (prow, pcol)).wait_recv()
        relay_copies(piece, send, recv, lambda copy: copy.start())

    def relay(i, late):
        for_relay(i, late, arrive_column)

    def load(which, i):
        if which == 0:
            return pltpu.make_async_copy(factor.at[i, 0, :, 0, 0, :], rows.at[i, side], load_sem.at[0, i])
        return pltpu.make_async_copy(matrix.at[i, 0, :, 0, 0, :], panel.at[i], load_sem.at[1, i])

    owner = top & (prow < 2) & (side <= prow)
    slot = 2 * (prow + side)

    def corner_copy(which, index):
        sent = panel.at[0] if which == 0 else rows.at[0, side]
        return remote(
            sent, corner.at[slot + which], corner_send.at[which, index], corner_recv.at[slot + which],
            (index // CORES, index % CORES),
        )

    def each_peer(act):
        def body(index, _):
            @pl.when(index != prow * CORES + side)
            def _():
                for which in range(2):
                    act(corner_copy(which, index))
            return 0
        lax.fori_loop(0, prows * CORES, body, 0)

    row_id = lax.broadcasted_iota(jnp.int32, (width, width), 0)
    col_id = lax.broadcasted_iota(jnp.int32, (width, width), 1)

    @pl.when(top)
    def _():
        def start_loads(i, _):
            load(1, i).start()
            load(0, i).start()
            return 0
        lax.fori_loop(0, row_tiles, start_loads, 0)
        load(1, 0).wait()
        load(0, 0).wait()

        @pl.when(owner)
        def _():
            each_peer(lambda copy: copy.start())
            corner[slot] = panel[0]
            corner[slot + 1] = rows[0, side]

        pass_whole(0, 0)
        emit(0, 0)

        def send_early(i, _):
            load(0, i).wait()
            pass_whole(i, 0)
            emit(i, 0)
            return 0
        lax.fori_loop(1, row_tiles, send_early, 0)

        def await_corner(index, _):
            @pl.when(jnp.logical_not(owner & ((index == slot) | (index == slot + 1))))
            def _():
                remote(
                    corner.at[index], corner.at[index], corner_send.at[0, 0], corner_recv.at[index], (prow, pcol)
                ).wait_recv()
            return 0
        lax.fori_loop(0, 6, await_corner, 0)

        levels = (width - 1).bit_length()

        def invert(step, _):
            lower = corner[1 + 4 * step]
            diagonal = row_id == col_id
            inverse[step] = jnp.where(diagonal, 1.0 / jnp.where(diagonal, lower, 1.0), 0.0)

            def level(bit, _):
                block = lax.shift_right_logical(row_id, bit)
                under = (block % 2 == 1) & (lax.shift_right_logical(col_id, bit) == block - 1)
                now = inverse[step]
                cross = jnp.where(under, corner[1 + 4 * step], 0.0)
                inverse[step] = now - dot(dot(now, cross), now)
                return 0
            lax.fori_loop(0, levels, level, 0)
            return 0
        lax.fori_loop(0, 2, invert, 0)

        def core_of(block, inv):
            symmetric = block + block.T - jnp.where(row_id == col_id, block, 0.0)
            inner = dot_trans(dot(inv, symmetric), inv)
            return 0.5 * (inner + inner.T)

        core[0] = core_of(corner[0], inverse[0])
        half[...] = dot_trans(corner[2], inverse[0]) - 0.5 * dot(corner[3], core[0])
        cross = dot_trans(half[...], corner[3]) + dot_trans(corner[3], half[...])
        corner[4] = corner[4] - jnp.where(row_id >= col_id, cross, 0.0)
        core[1] = core_of(corner[4], inverse[1])

        @pl.when(owner)
        def _():
            each_peer(lambda copy: copy.wait_send())

    @pl.when(jnp.logical_not(top))
    def _():
        def pass_early(i, _):
            pass_whole(i, 0)
            emit(i, 0)
            relay(i - early_lag, 0)
            return 0
        lax.fori_loop(0, row_tiles, pass_early, 0)

    def reduce_tile(i):
        @pl.when(i > 0)
        def _():
            load(1, i).wait()

        @pl.when(side == 1)
        def _():
            for late in range(2):
                side_copy(i, late, 2 * late).wait_recv()
            panel[i] = (
                panel[i] - dot_trans(rows[i, 2], corner[3]) - dot_trans(rows[i, 0], half[...])
            )

        shared = dot(rows[i, side], core[side])
        halfway = dot_trans(panel[i], inverse[side]) - 0.5 * shared
        rows[i, side + 2] = halfway
        tile = i * prows + prow
        lower = jnp.where(row_id >= col_id, core[side], 0.0)
        final = halfway - 0.5 * shared
        final = jnp.where(tile > side, final, jnp.where(tile == side, lower, 0.0))
        panel[i] = final

    early = early_pairs(row_tiles)

    def row_ready(i):
        @pl.when(jnp.logical_not(top & (side == 1)))
        def _():
            for late in range(2):
                side_copy(i, late, 1 - side + 2 * late).wait_recv()

        @pl.when(i >= 2 * early)
        def _():
            pltpu.make_async_copy(rows.at[i], row_out.at[i - 2 * early], row_sem.at[i]).start()

    def column_out(j):
        return (
            pltpu.make_async_copy(col_high.at[j], high_out.at[j], column_sem.at[0, j]),
            pltpu.make_async_copy(col_low.at[j], low_out.at[j], column_sem.at[1, j]),
        )

    def column_ready(i):
        j = (i - first_tile) // ratio

        @pl.when((i >= first_tile) & (i < row_tiles) & ((i - first_tile) % ratio == 0))
        def _():
            @pl.when(prow == source)
            def _():
                split_column(rows.at[i], col_high.at[j], col_low.at[j])

            @pl.when(prow != source)
            def _():
                split_column(cols.at[j], col_high.at[j], col_low.at[j])

            @pl.when(j >= 1)
            def _():
                for copy in column_out(j - 1):
                    copy.start()

    def each_tile(pair, act):
        def body(j, _):
            for place in range(2):
                act(j, place)
            return 0
        lax.fori_loop(0, pair_columns(pair, ratio), body, 0)

    def tile_in(pair, j, place):
        return pltpu.make_async_copy(
            matrix.at[2 * pair + place, 0, :, j, 0, :], tiles.at[pair % 2, j, place], tile_load.at[pair % 2, j, place]
        )

    def tile_done(pair, j, place):
        return pltpu.make_async_copy(
            tiles.at[pair % 2, j, place], done_out.at[pair, j, place], tile_out.at[pair % 2, j, place]
        )

    def work(i, part):
        step = i - 1 - work_lag
        pair = step // 2
        slot = step % 2 * PARTS + part
        last = pair_columns(pair, ratio) - 1
        j = jnp.where(slot == 2 * PARTS - 1, last, slot)

        @pl.when((step >= 0) & (pair < early))
        def _():
            @pl.when(slot == 0)
            def _():
                @pl.when(pair >= 1)
                def _():
                    each_tile(pair - 1, lambda j, place: tile_done(pair - 1, j, place).wait())

                @pl.when(pair + 1 < early)
                def _():
                    each_tile(pair + 1, lambda j, place: tile_in(pair + 1, j, place).start())
                split_rows(rows.at[2 * pair], rows.at[2 * pair + 1], row_high, row_low)

            @pl.when((slot < last) | (slot == 2 * PARTS - 1))
            def _():
                for place in range(2):
                    tile_in(pair, j, place).wait()

                @pl.when((pcol >= 2) | (j > 0))
                def _():
                    subtract_update(
                        tiles.at[pair % 2, j], row_high, row_low, col_high.at[j], col_low.at[j],
                        2 * pair * prows + prow, prows, j * pcols + pcol,
                    )
                for place in range(2):
                    tile_done(pair, j, place).start()

    each_tile(0, lambda j, place: tile_in(0, j, place).start())

    @pl.when(top)
    def _():
        def reduce_step(i, _):
            @pl.when(i < row_tiles)
            def _():
                reduce_tile(i)

            @pl.when(i >= 1)
            def _():
                pass_whole(i - 1, 1)
                emit(i - 1, 1)
            return 0
        lax.fori_loop(0, row_tiles + 1, reduce_step, 0)

    def late_column(tile):
        relay(tile, 1)
        column_ready(tile)

    def drain(i, late):
        @pl.when(plane < depth - 1)
        def _():
            whole = rows.at[i, side + CORES * late]
            remote(whole, whole, down_send.at[i, late], down_recv.at[i, late, 0], (prow, pcol + CORES)).wait_send()

        if late:
            @pl.when(i >= row_tiles - ratio)
            def _():
                for part in range(PARTS - 1):
                    for_columns(i, late, part, lambda copy: copy.wait_send())
        for_columns(i, late, PARTS - 1, lambda copy: copy.wait_send())
        side_copy(i, late, side + 2 * late).wait_send()
        for_relay(
            i, late,
            lambda kind, piece, send, recv: relay_copies(piece, send, recv, lambda copy: copy.wait_send()),
        )

    def last_column(tile, _):
        late_column(tile)
        return 0

    def late_step(i, _):
        here = jnp.logical_not(top) & (i >= 1) & (i <= row_tiles)

        @pl.when(top & (i < row_tiles))
        def _():
            relay(i, 0)

        @pl.when(jnp.logical_not(top) & (i < early_lag))
        def _():
            relay(row_tiles - early_lag + i, 0)

        @pl.when(bridge & (i == row_tiles + 1))
        def _():
            lax.fori_loop(row_tiles - NEAR, row_tiles, last_column, 0)

        def part_step(part, _):
            @pl.when(here)
            def _():
                pass_down(i - 1, 1, part)

                @pl.when(part == PARTS - 1)
                def _():
                    emit(i - 1, 1)

            @pl.when((part == PARTS - 1) & jnp.logical_not(bridge & (i > row_tiles)))
            def _():
                late_column(i - 1 - lag)
            work(i, part)
            return 0
        lax.fori_loop(0, PARTS, part_step, 0)

        @pl.when((i >= 2) & (i < row_tiles + 2))
        def _():
            row_ready(i - 2)

        @pl.when(i < row_tiles)
        def _():
            drain(i, 0)

        @pl.when((i >= SENT) & (i < row_tiles + SENT))
        def _():
            drain(i - SENT, 1)
        return 0
    steps = max(row_tiles + 2, 2 * early + work_lag + 1)
    lax.fori_loop(0, steps, late_step, 0)

    @pl.when(jnp.logical_not(bridge))
    def _():
        lax.fori_loop(steps - 1 - lag, row_tiles, last_column, 0)
    for copy in column_out(col_tiles - 1):
        copy.start()
    each_tile(early - 1, lambda j, place: tile_done(early - 1, j, place).wait())

    fin_copy = pltpu.make_async_copy(panel, fin_out, out_sem)

    @pl.when(top)
    def _():
        fin_copy.start()

    def drain_rest(i, _):
        drain(i, 1)
        return 0
    lax.fori_loop(max(0, steps - SENT), row_tiles, drain_rest, 0)

    def drain_out(i, _):
        @pl.when(i >= 2 * early)
        def _():
            pltpu.make_async_copy(rows.at[i], row_out.at[i - 2 * early], row_sem.at[i]).wait()
        return 0
    lax.fori_loop(0, row_tiles, drain_out, 0)

    def drain_column(j, _):
        for copy in column_out(j):
            copy.wait()
        return 0
    lax.fori_loop(0, col_tiles, drain_column, 0)

    @pl.when(top)
    def _():
        fin_copy.wait()


def update_kernel(
    prows, pcols, matrix, row_in, high_in, low_in, fin_in, done_in, out,
    rows, row_high, row_low, col_high, col_low, tiles, zeros,
    row_sem, col_sem, in_sem, out_sem,
):
    row_tiles, col_tiles, width, _ = tiles.shape
    ratio = pcols // prows
    early = early_pairs(row_tiles)
    pairs = row_tiles // 2
    prow = lax.axis_index("prow")
    pcol = lax.axis_index("pcol")
    zeros[...] = jnp.zeros_like(zeros)

    def col_copies(j):
        return (
            pltpu.make_async_copy(high_in.at[j], col_high.at[j], col_sem.at[0, j]),
            pltpu.make_async_copy(low_in.at[j], col_low.at[j], col_sem.at[1, j]),
        )

    def row_copy(i):
        return pltpu.make_async_copy(row_in.at[i], rows.at[i], row_sem.at[i])

    def live(i, j):
        return j * pcols + pcol <= i * prows + prow

    def is_fixed(j):
        return (pcol < 2) & (j == 0)

    def start_in(i, j):
        @pl.when(live(i, j))
        def _():
            @pl.when(is_fixed(j))
            def _():
                pltpu.make_async_copy(fin_in.at[i], tiles.at[i, j], in_sem.at[i, j]).start()

            @pl.when(jnp.logical_not(is_fixed(j)) & (i < 2 * early))
            def _():
                pltpu.make_async_copy(done_in.at[i // 2, j, i % 2], tiles.at[i, j], in_sem.at[i, j]).start()

            @pl.when(jnp.logical_not(is_fixed(j)) & (i >= 2 * early))
            def _():
                pltpu.make_async_copy(matrix.at[i, 0, :, j, 0, :], tiles.at[i, j], in_sem.at[i, j]).start()

    def wait_in(i, j):
        @pl.when(live(i, j))
        def _():
            pltpu.make_async_copy(fin_in.at[i], tiles.at[i, j], in_sem.at[i, j]).wait()

    def out_copy(i, j):
        return pltpu.make_async_copy(tiles.at[i, j], out.at[i, 0, :, j, 0, :], out_sem.at[i, j])

    def start_out(i, j):
        @pl.when(live(i, j))
        def _():
            out_copy(i, j).start()

    def over_columns(i, count, act):
        def body(j, _):
            act(i, j)
            return 0
        lax.fori_loop(0, count, body, 0)

    def load_row(i, _):
        over_columns(i, col_tiles, start_in)
        return 0

    def zero_row(i):
        def body(j, _):
            @pl.when(jnp.logical_not(live(i, j)))
            def _():
                pltpu.make_async_copy(zeros, out.at[i, 0, :, j, 0, :], out_sem.at[i, j]).start()
            return 0
        lax.fori_loop(0, col_tiles, body, 0)

    for i in range(2):
        row_copy(i).start()
    for copy in col_copies(0):
        copy.start()
    lax.fori_loop(2 * early, 2 * early + 2, load_row, 0)
    for j in range(1, col_tiles):
        for copy in col_copies(j):
            copy.start()
    for i in range(2, row_tiles - 2 * early):
        row_copy(i).start()
    lax.fori_loop(2 * early + 2, row_tiles, load_row, 0)

    def feed(step):
        for place in range(2):
            i = 2 * step + place

            @pl.when(i < row_tiles)
            def _():
                @pl.when(i < 2 * early)
                def _():
                    load_row(i, 0)
                zero_row(i)

    def hand_on(i):
        @pl.when((i >= 0) & (i < 2 * early))
        def _():
            over_columns(i, col_tiles, wait_in)
            over_columns(i, col_tiles, start_out)

    def hand_pair(step):
        for place in range(2):
            hand_on(2 * step + place)

    def pair_step(pair, passed):
        for place in range(2):
            row_copy(2 * (pair - early) + place).wait()
        split_rows(
            rows.at[2 * (pair - early)], rows.at[2 * (pair - early) + 1], row_high, row_low
        )
        count = pair_columns(pair, ratio)
        old = jnp.where(pair == early, 0, pair_columns(pair - 1, ratio))

        def tile_step(j, _):
            feed(passed + j)

            @pl.when(j >= old)
            def _():
                for copy in col_copies(j):
                    copy.wait()
            for place in range(2):
                wait_in(2 * pair + place, j)

            @pl.when(jnp.logical_not(is_fixed(j)))
            def _():
                subtract_update(
                    tiles.at[pl.ds(2 * pair, 2), j], row_high, row_low, col_high.at[j], col_low.at[j],
                    2 * pair * prows + prow, prows, j * pcols + pcol,
                )
            for place in range(2):
                start_out(2 * pair + place, j)
            hand_pair(passed + j - 2)
            return 0
        lax.fori_loop(0, count, tile_step, 0)
        return passed + count
    passed = lax.fori_loop(early, pairs, pair_step, 0)

    def feed_rest(step, _):
        feed(step)
        return 0
    lax.fori_loop(passed, pairs, feed_rest, 0)

    def hand_rest(step, _):
        hand_pair(step)
        return 0
    lax.fori_loop(jnp.maximum(passed - 2, 0), pairs, hand_rest, 0)

    def finish(i, _):
        def body(j, _):
            out_copy(i, j).wait()
            return 0
        lax.fori_loop(0, col_tiles, body, 0)
        return 0
    lax.fori_loop(0, row_tiles, finish, 0)


def on_device(matrix, factor):
    row_tiles, _, width, col_tiles, _, _ = matrix.shape
    prows = lax.axis_size("prow")
    pcols = lax.axis_size("pcol")
    tile = (width, width)
    f32 = jnp.float32
    anywhere = pl.BlockSpec(memory_space=pl.ANY)
    dma = pltpu.SemaphoreType.DMA
    early = early_pairs(row_tiles)
    reach = pair_columns(early - 1, pcols // prows)
    late_rows = row_tiles - 2 * early
    bf16 = jnp.bfloat16
    lanes = lanes_of(prows)
    row_all, high_all, low_all, fin, done = pl.pallas_call(
        functools.partial(gather_kernel, prows, pcols),
        out_shape=(
            jax.ShapeDtypeStruct((late_rows, 4) + tile, f32),
            jax.ShapeDtypeStruct((col_tiles, width, 4 * width), bf16),
            jax.ShapeDtypeStruct((col_tiles, width, 4 * width), bf16),
            jax.ShapeDtypeStruct((row_tiles,) + tile, f32),
            jax.ShapeDtypeStruct((early, reach, 2) + tile, f32),
        ),
        in_specs=[anywhere, anywhere],
        out_specs=(anywhere,) * 5,
        scratch_shapes=[
            pltpu.VMEM((row_tiles, 4) + tile, f32),
            pltpu.VMEM((col_tiles, 4) + tile, f32),
            pltpu.VMEM((row_tiles,) + tile, f32),
            pltpu.VMEM((6,) + tile, f32),
            pltpu.VMEM((2,) + tile, f32),
            pltpu.VMEM((2,) + tile, f32),
            pltpu.VMEM(tile, f32),
            pltpu.VMEM((2 * width, 4 * width), bf16),
            pltpu.VMEM((2 * width, 4 * width), bf16),
            pltpu.VMEM((col_tiles, width, 4 * width), bf16),
            pltpu.VMEM((col_tiles, width, 4 * width), bf16),
            pltpu.VMEM((2, reach, 2) + tile, f32),
            dma((2, row_tiles)),
            dma((row_tiles, 2, PARTS)),
            dma((row_tiles, 2)),
            dma((col_tiles, 4)),
            dma((2, PARTS)),
            dma((6,)),
            dma((2, prows * CORES)),
            dma((row_tiles, 2)),
            dma((row_tiles, 2)),
            dma((lanes, col_tiles, 2)),
            dma((lanes, PARTS)),
            dma((lanes, col_tiles, 4)),
            dma((lanes, 2, PARTS)),
            dma,
            dma((row_tiles,)),
            dma((2, col_tiles)),
            dma((2, reach, 2)),
            dma((2, reach, 2)),
        ],
        compiler_params=pltpu.CompilerParams(collective_id=0, has_side_effects=True, vmem_limit_bytes=LIMIT),
        name="gather",
    )(matrix, factor)
    return pl.pallas_call(
        functools.partial(update_kernel, prows, pcols),
        out_shape=jax.ShapeDtypeStruct(matrix.shape, f32),
        in_specs=[anywhere] * 6,
        out_specs=anywhere,
        scratch_shapes=[
            pltpu.VMEM((late_rows, 4) + tile, f32),
            pltpu.VMEM((2 * width, 4 * width), bf16),
            pltpu.VMEM((2 * width, 4 * width), bf16),
            pltpu.VMEM((col_tiles, width, 4 * width), bf16),
            pltpu.VMEM((col_tiles, width, 4 * width), bf16),
            pltpu.VMEM((row_tiles, col_tiles) + tile, f32),
            pltpu.VMEM(tile, f32),
            dma((late_rows,)),
            dma((2, col_tiles)),
            dma((row_tiles, col_tiles)),
            dma((row_tiles, col_tiles)),
        ],
        compiler_params=pltpu.CompilerParams(vmem_limit_bytes=LIMIT),
        name="update",
    )(matrix, row_all, high_all, low_all, fin, done)


def solution(mesh):
    placed = P(None, "prow", None, None, "pcol", None)
    return jax.shard_map(on_device, mesh=mesh, in_specs=(placed, placed), out_specs=placed, check_vma=False)
```
